8 devices in a mesh: pp: 2 (over z, y), dp: 4 (over x, core).
Axes of the slice: x: 2, y: 2, z: 1, core: 2. Of those that a mesh axis runs over, the one named last changes fastest.
Arguments:
- act_in: bfloat16 [4, 24, 256, 768], P(None, 'dp')
- loss_seed: bfloat16 [4, 24, 256, 768], P(None, 'dp')
- w_qkv: bfloat16 [2, 768, 36, 64], P('pp', 'dp')
- w_proj: bfloat16 [2, 768, 768], P('pp', 'dp')
- w_up: bfloat16 [2, 768, 3072], P('pp', 'dp')
- w_down: bfloat16 [2, 3072, 768], P('pp', 'dp')
Outputs:
- output 1: float32 [2, 768, 36, 64], P('pp', 'dp')
- output 2: float32 [2, 768, 768], P('pp', 'dp')
- output 3: float32 [2, 768, 3072], P('pp', 'dp')
- output 4: float32 [2, 3072, 768], P('pp', 'dp')
- output 5: bfloat16 [4, 24, 256, 768], P(None, 'dp', 'pp')
All inputs are finite; a program needn't handle non-finite values.
Results may differ from the reference program's by a relative error of at most 0.02.
Values are sent between devices in bfloat16 or wider.
A program may use at most 1 GiB of HBM per device.

```python
import jax
import jax.numpy as jnp
from jax import lax

MICROBATCHES = 4
DP_SIZE = 4
BATCH_DEV = 6
SEQ_LEN = 256
D_MODEL = 768
NUM_HEADS = 12
TOTAL_LAYERS = 2

HEAD_DIM = D_MODEL // NUM_HEADS
ROWS_ALL = DP_SIZE * BATCH_DEV
NORM_EPS = 1e-6


def setup_inputs(seed: int = 0) -> dict:
    key_list = jax.random.split(jax.random.key(seed), 6)
    act_shape = (MICROBATCHES, ROWS_ALL, SEQ_LEN, D_MODEL)
    seed_scale = (MICROBATCHES * ROWS_ALL * SEQ_LEN) ** -0.5
    act_in = jax.random.normal(key_list[0], act_shape, jnp.float32).astype(jnp.bfloat16)
    loss_seed = (jax.random.normal(key_list[1], act_shape, jnp.float32) * seed_scale).astype(jnp.bfloat16)
    w_qkv = (jax.random.normal(key_list[2], (TOTAL_LAYERS, D_MODEL, 3 * NUM_HEADS, HEAD_DIM), jnp.float32) * D_MODEL ** -0.5).astype(jnp.bfloat16)
    w_proj = (jax.random.normal(key_list[3], (TOTAL_LAYERS, D_MODEL, D_MODEL), jnp.float32) * D_MODEL ** -0.5).astype(jnp.bfloat16)
    w_up = (jax.random.normal(key_list[4], (TOTAL_LAYERS, D_MODEL, 4 * D_MODEL), jnp.float32) * D_MODEL ** -0.5).astype(jnp.bfloat16)
    w_down = (jax.random.normal(key_list[5], (TOTAL_LAYERS, 4 * D_MODEL, D_MODEL), jnp.float32) * (4 * D_MODEL) ** -0.5).astype(jnp.bfloat16)
    return {'act_in': act_in, 'loss_seed': loss_seed, 'w_qkv': w_qkv, 'w_proj': w_proj, 'w_up': w_up, 'w_down': w_down}


def bf16_cast(values):
    return values.astype(jnp.bfloat16).astype(jnp.float32)


def rms_norm(hidden):
    return hidden * lax.rsqrt(jnp.mean(hidden * hidden, axis=-1, keepdims=True) + NORM_EPS)


def layer_apply(hidden, layer_w):
    w_qkv, w_proj, w_up, w_down = layer_w
    hid_f32 = hidden.astype(jnp.float32)
    normed = bf16_cast(rms_norm(hid_f32))
    qkv_act = bf16_cast(jnp.einsum('bsd,dnh->bsnh', normed, w_qkv))
    q_heads = qkv_act[:, :, :NUM_HEADS]
    k_heads = qkv_act[:, :, NUM_HEADS:2 * NUM_HEADS]
    v_heads = qkv_act[:, :, 2 * NUM_HEADS:]
    scores = jnp.einsum('bqnh,bknh->bnqk', q_heads, k_heads) * HEAD_DIM ** -0.5
    causal = jnp.arange(SEQ_LEN)[:, None] >= jnp.arange(SEQ_LEN)[None, :]
    prob_bf = bf16_cast(jax.nn.softmax(jnp.where(causal, scores, -1e30), axis=-1))
    attn_out = bf16_cast(jnp.einsum('bnqk,bknh->bqnh', prob_bf, v_heads))
    attn_flat = attn_out.reshape(hidden.shape)
    mid_f32 = bf16_cast(hid_f32 + jnp.einsum('bse,ed->bsd', attn_flat, w_proj))
    normed2 = bf16_cast(rms_norm(mid_f32))
    up_act = bf16_cast(jnp.einsum('bsd,df->bsf', normed2, w_up))
    gelu_out = bf16_cast(jax.nn.gelu(up_act, approximate=True))
    return (mid_f32 + jnp.einsum('bsf,fd->bsd', gelu_out, w_down)).astype(jnp.bfloat16)


def stack_apply(weight_set, hidden):
    def layer_step(hidden_now, layer_w):
        return layer_apply(hidden_now, layer_w), None
    final_out, _ = lax.scan(jax.checkpoint(layer_step), hidden, weight_set)
    return final_out


def reference(act_in, loss_seed, w_qkv, w_proj, w_up, w_down):
    weights = (w_qkv.astype(jnp.float32), w_proj.astype(jnp.float32), w_up.astype(jnp.float32), w_down.astype(jnp.float32))
    rows_in = act_in.reshape(MICROBATCHES * DP_SIZE, BATCH_DEV, SEQ_LEN, D_MODEL)
    rows_seed = loss_seed.reshape(MICROBATCHES * DP_SIZE, BATCH_DEV, SEQ_LEN, D_MODEL)

    def row_step(grad_sum, row_pair):
        hidden, cotangent = row_pair
        rows_out, pull_back = jax.vjp(lambda weight_set: stack_apply(weight_set, hidden), weights)
        row_grads = pull_back(cotangent)[0]
        return tuple(acc_part + grad_part for acc_part, grad_part in zip(grad_sum, row_grads)), rows_out

    zero_grads = tuple(jnp.zeros_like(w_full) for w_full in weights)
    grad_sum, outs_all = lax.scan(row_step, zero_grads, (rows_in, rows_seed))
    act_out = outs_all.reshape(MICROBATCHES, ROWS_ALL, SEQ_LEN, D_MODEL)
    return grad_sum[0], grad_sum[1], grad_sum[2], grad_sum[3], act_out
```

```python
import functools
import math

import jax
import jax.numpy as jnp
from jax import lax
from jax.experimental import pallas as pl
from jax.experimental.pallas import tpu as pltpu
from jax.sharding import PartitionSpec as P

NORM_EPS = 1e-6
BF = jnp.bfloat16
F32 = jnp.float32
VMEM_LIMIT = 62 * 1024 * 1024
GELU_C = math.sqrt(2.0 / math.pi)
NN = (((1,), (0,)), ((), ()))
NT = (((1,), (1,)), ((), ()))
TN = (((0,), (0,)), ((), ()))


def dot(lhs, rhs, dims=NN):
    return lax.dot_general(lhs, rhs, dims, preferred_element_type=F32)


def rms_scale(hid_f32):
    return lax.rsqrt(jnp.mean(hid_f32 * hid_f32, axis=-1, keepdims=True) + NORM_EPS)


def rms_pull(hid_f32, scale, ct):
    inner = jnp.mean(ct * hid_f32, axis=-1, keepdims=True)
    return scale * (ct - hid_f32 * (scale * scale * inner))


def gelu_parts(pre):
    sq = pre * pre
    th = jnp.tanh(pre * (GELU_C + (GELU_C * 0.044715) * sq))
    half = 0.5 + 0.5 * th
    return sq, th, half


def head_masks(value):
    lane = lax.broadcasted_iota(jnp.int32, (1, 128), 1)
    low = jnp.where(lane < 64, value, 0.0).astype(BF)
    high = jnp.where(lane < 64, 0.0, value).astype(BF)
    return low, high


def causal_tile():
    return lax.broadcasted_iota(jnp.int32, (128, 128), 0) <= lax.broadcasted_iota(jnp.int32, (128, 128), 1)


def attn_fwd_kernel(h_ref, w_ref, qkv_ref, attn_ref, lse_ref):
    d_model = h_ref.shape[-1]
    hid = h_ref[...].astype(F32)
    normed = (hid * rms_scale(hid)).astype(BF)
    for part in range(3):
        cols = slice(part * d_model, (part + 1) * d_model)
        qkv_ref[:, cols] = dot(normed, w_ref[:, cols]).astype(BF)
    masks = head_masks(0.125)
    keep = causal_tile()
    zero_tile = jnp.zeros((128, 128), BF)
    for pair in range(d_model // 128):
        base = pair * 128
        q_pair = qkv_ref[:, base:base + 128]
        k_pair = qkv_ref[:, d_model + base:d_model + base + 128]
        v_tr = qkv_ref[:, 2 * d_model + base:2 * d_model + base + 128].T
        outs = []
        for sub in range(2):
            scores = dot(k_pair, q_pair * masks[sub], NT)
            s00 = jnp.where(keep, scores[:128, :128], -1e30)
            s01 = scores[:128, 128:]
            s11 = jnp.where(keep, scores[128:, 128:], -1e30)
            top0 = jnp.max(s00, axis=0, keepdims=True)
            top1 = jnp.max(jnp.maximum(s01, s11), axis=0, keepdims=True)
            e00 = jnp.exp(s00 - top0)
            e01 = jnp.exp(s01 - top1)
            e11 = jnp.exp(s11 - top1)
            sum0 = jnp.sum(e00, axis=0, keepdims=True)
            sum1 = jnp.sum(e01 + e11, axis=0, keepdims=True)
            inv0 = 1.0 / sum0
            inv1 = 1.0 / sum1
            prob = jnp.concatenate([
                jnp.concatenate([(e00 * inv0).astype(BF), (e01 * inv1).astype(BF)], axis=1),
                jnp.concatenate([zero_tile, (e11 * inv1).astype(BF)], axis=1)], axis=0)
            lse_ref[2 * pair + sub:2 * pair + sub + 1, :] = jnp.concatenate([top0 + jnp.log(sum0), top1 + jnp.log(sum1)], axis=1)
            outs.append(dot(v_tr[sub * 64:(sub + 1) * 64], prob))
        attn_ref[:, base:base + 128] = jnp.concatenate(outs, axis=0).T.astype(BF)


def attn_forward(hidden, w_qkv):
    seqs, seq_len, d_model = hidden.shape
    heads = d_model // 64
    flops = 2 * seqs * seq_len * d_model * 3 * d_model + 8 * seqs * heads * seq_len * seq_len * 128
    return pl.pallas_call(
        attn_fwd_kernel,
        grid=(seqs,),
        in_specs=[
            pl.BlockSpec((None, seq_len, d_model), lambda i: (i, 0, 0)),
            pl.BlockSpec((d_model, 3 * d_model), lambda i: (0, 0), pipeline_mode=pl.Buffered(1)),
        ],
        out_specs=[
            pl.BlockSpec((None, seq_len, 3 * d_model), lambda i: (i, 0, 0)),
            pl.BlockSpec((None, seq_len, d_model), lambda i: (i, 0, 0)),
            pl.BlockSpec((None, heads, seq_len), lambda i: (i, 0, 0)),
        ],
        out_shape=[
            jax.ShapeDtypeStruct((seqs, seq_len, 3 * d_model), BF),
            jax.ShapeDtypeStruct((seqs, seq_len, d_model), BF),
            jax.ShapeDtypeStruct((seqs, heads, seq_len), F32),
        ],
        cost_estimate=pl.CostEstimate(flops=flops, bytes_accessed=40 << 20, transcendentals=0),
        compiler_params=pltpu.CompilerParams(vmem_limit_bytes=VMEM_LIMIT),
        name='attn_fwd',
    )(hidden, w_qkv)


def mlp_fwd_kernel(h_ref, attn_ref, wp_ref, wu_ref, wd_ref, mid_ref, up_ref, out_ref):
    d_model = h_ref.shape[-1]
    mid = (h_ref[...].astype(F32) + dot(attn_ref[...], wp_ref[...])).astype(BF)
    mid_ref[...] = mid
    mid = mid.astype(F32)
    normed = (mid * rms_scale(mid)).astype(BF)
    total = mid
    for part in range(wu_ref.shape[1] // d_model):
        cols = slice(part * d_model, (part + 1) * d_model)
        up = dot(normed, wu_ref[:, cols]).astype(BF)
        up_ref[:, cols] = up
        pre = up.astype(F32)
        act = (pre * gelu_parts(pre)[2]).astype(BF)
        total = total + dot(act, wd_ref[cols, :])
    out_ref[...] = total.astype(BF)


def mlp_forward(hidden, attn, w_proj, w_up, w_down, rows=512):
    tokens, d_model = hidden.shape
    d_ff = w_up.shape[1]
    flops = 2 * tokens * d_model * (d_model + 2 * d_ff)
    row_spec = pl.BlockSpec((rows, d_model), lambda i: (i, 0))
    whole = lambda shape: pl.BlockSpec(shape, lambda i: (0, 0), pipeline_mode=pl.Buffered(1))
    return pl.pallas_call(
        mlp_fwd_kernel,
        grid=(tokens // rows,),
        in_specs=[row_spec, row_spec, whole(w_proj.shape), whole(w_up.shape), whole(w_down.shape)],
        out_specs=[row_spec, pl.BlockSpec((rows, d_ff), lambda i: (i, 0)), row_spec],
        out_shape=[
            jax.ShapeDtypeStruct((tokens, d_model), BF),
            jax.ShapeDtypeStruct((tokens, d_ff), BF),
            jax.ShapeDtypeStruct((tokens, d_model), BF),
        ],
        cost_estimate=pl.CostEstimate(flops=flops, bytes_accessed=50 << 20, transcendentals=0),
        compiler_params=pltpu.CompilerParams(vmem_limit_bytes=VMEM_LIMIT),
        name='mlp_fwd',
    )(hidden, attn, w_proj, w_up, w_down)


def mlp_bwd_kernel(ct_ref, up_ref, mid_ref, attn_ref, wp_ref, wu_ref, wd_ref,
                   ct_mid_ref, ct_attn_ref, gd_out, gu_out, gp_out, gd_acc, gu_acc, gp_acc, sems):
    step = pl.program_id(0)
    last = pl.num_programs(0) - 1
    d_model = ct_ref.shape[-1]
    parts = wu_ref.shape[1] // d_model

    @pl.when(step == 0)
    def _():
        gd_acc[...] = jnp.zeros_like(gd_acc)
        gu_acc[...] = jnp.zeros_like(gu_acc)
        gp_acc[...] = jnp.zeros_like(gp_acc)

    def down_copy(part):
        sl = pl.ds(part * d_model, d_model)
        return pltpu.make_async_copy(gd_acc.at[sl, :], gd_out.at[sl, :], sems.at[part])

    def up_copy(part):
        sl = pl.ds(part * d_model, d_model)
        return pltpu.make_async_copy(gu_acc.at[:, sl], gu_out.at[:, sl], sems.at[parts + part])

    proj_copy = pltpu.make_async_copy(gp_acc, gp_out, sems.at[2 * parts])

    ct = ct_ref[...]
    mid = mid_ref[...].astype(F32)
    scale = rms_scale(mid)
    normed = (mid * scale).astype(BF)
    ct_norm = jnp.zeros(mid.shape, F32)
    for part in range(parts):
        cols = slice(part * d_model, (part + 1) * d_model)
        pre = up_ref[:, cols].astype(F32)
        sq, th, half = gelu_parts(pre)
        act = (pre * half).astype(BF)
        slope = half + (0.5 * pre) * (1.0 - th * th) * (GELU_C + (3.0 * 0.044715 * GELU_C) * sq)
        gd_acc[cols, :] += dot(act, ct, TN)
        ct_act = dot(ct, wd_ref[cols, :], NT).astype(BF).astype(F32)
        ct_up = (ct_act * slope).astype(BF)
        gu_acc[:, cols] += dot(normed, ct_up, TN)
        ct_norm = ct_norm + dot(ct_up, wu_ref[:, cols], NT)

        @pl.when(step == last)
        def _():
            down_copy(part).start()
            up_copy(part).start()

    ct_norm = ct_norm.astype(BF).astype(F32)
    ct_mid = (ct.astype(F32) + rms_pull(mid, scale, ct_norm)).astype(BF)
    ct_mid_ref[...] = ct_mid
    gp_acc[...] += dot(attn_ref[...], ct_mid, TN)
    ct_attn_ref[...] = dot(ct_mid, wp_ref[...], NT).astype(BF)

    @pl.when(step == last)
    def _():
        proj_copy.start()
        for part in range(parts):
            down_copy(part).wait()
            up_copy(part).wait()
        proj_copy.wait()


def mlp_backward(ct, up, mid, attn, w_proj, w_up, w_down, rows=512):
    tokens, d_model = ct.shape
    d_ff = w_up.shape[1]
    parts = d_ff // d_model
    flops = 4 * tokens * d_model * (d_model + 2 * d_ff)
    row_spec = pl.BlockSpec((rows, d_model), lambda i: (i, 0))
    whole = lambda shape: pl.BlockSpec(shape, lambda i: (0, 0), pipeline_mode=pl.Buffered(1))
    hbm = pl.BlockSpec(memory_space=pl.ANY)
    return pl.pallas_call(
        mlp_bwd_kernel,
        grid=(tokens // rows,),
        in_specs=[row_spec, pl.BlockSpec((rows, d_ff), lambda i: (i, 0)), row_spec, row_spec,
                  whole(w_proj.shape), whole(w_up.shape), whole(w_down.shape)],
        out_specs=[row_spec, row_spec, hbm, hbm, hbm],
        out_shape=[
            jax.ShapeDtypeStruct((tokens, d_model), BF),
            jax.ShapeDtypeStruct((tokens, d_model), BF),
            jax.ShapeDtypeStruct((d_ff, d_model), F32),
            jax.ShapeDtypeStruct((d_model, d_ff), F32),
            jax.ShapeDtypeStruct((d_model, d_model), F32),
        ],
        scratch_shapes=[
            pltpu.VMEM((d_ff, d_model), F32),
            pltpu.VMEM((d_model, d_ff), F32),
            pltpu.VMEM((d_model, d_model), F32),
            pltpu.SemaphoreType.DMA((2 * parts + 1,)),
        ],
        cost_estimate=pl.CostEstimate(flops=flops, bytes_accessed=70 << 20, transcendentals=0),
        compiler_params=pltpu.CompilerParams(vmem_limit_bytes=VMEM_LIMIT),
        name='mlp_bwd',
    )(ct, up, mid, attn, w_proj, w_up, w_down)


def attn_bwd_kernel(with_input, *refs):
    if with_input:
        h_ref, qkv_ref, lse_ref, ct_attn_ref, ct_mid_ref, w_ref, ct_h_ref, g_out, dqkv, g_acc, sem = refs
    else:
        h_ref, qkv_ref, lse_ref, ct_attn_ref, g_out, dqkv, g_acc, sem = refs
    step = pl.program_id(0)
    last = pl.num_programs(0) - 1
    d_model = h_ref.shape[-1]

    @pl.when(step == 0)
    def _():
        g_acc[...] = jnp.zeros_like(g_acc)

    q_masks = head_masks(0.125)
    o_masks = head_masks(1.0)
    keep = causal_tile()
    zero_tile = jnp.zeros((128, 128), BF)

    def square(t00, t01, t11):
        return jnp.concatenate([
            jnp.concatenate([t00.astype(BF), t01.astype(BF)], axis=1),
            jnp.concatenate([zero_tile, t11.astype(BF)], axis=1)], axis=0)

    for pair in range(d_model // 128):
        base = pair * 128
        q_pair = qkv_ref[:, base:base + 128]
        k_pair = qkv_ref[:, d_model + base:d_model + base + 128]
        v_pair = qkv_ref[:, 2 * d_model + base:2 * d_model + base + 128]
        o_pair = ct_attn_ref[:, base:base + 128]
        k_tr = k_pair.T
        dq_parts = []
        dk_pair = None
        dv_pair = None
        for sub in range(2):
            q_sub = q_pair * q_masks[sub]
            o_sub = o_pair * o_masks[sub]
            scores = dot(k_pair, q_sub, NT)
            d_prob = dot(v_pair, o_sub, NT)
            lse0 = lse_ref[2 * pair + sub:2 * pair + sub + 1, :128]
            lse1 = lse_ref[2 * pair + sub:2 * pair + sub + 1, 128:]
            p00 = jnp.exp(jnp.where(keep, scores[:128, :128] - lse0, -1e30))
            p01 = jnp.exp(scores[:128, 128:] - lse1)
            p11 = jnp.exp(jnp.where(keep, scores[128:, 128:] - lse1, -1e30))
            d00 = d_prob[:128, :128].astype(BF).astype(F32)
            d01 = d_prob[:128, 128:].astype(BF).astype(F32)
            d11 = d_prob[128:, 128:].astype(BF).astype(F32)
            m0 = jnp.sum(p00 * d00, axis=0, keepdims=True)
            m1 = jnp.sum(p01 * d01 + p11 * d11, axis=0, keepdims=True)
            prob = square(p00, p01, p11)
            d_score = square(p00 * (d00 - m0), p01 * (d01 - m1), p11 * (d11 - m1))
            dv_sub = dot(prob, o_sub)
            dk_sub = dot(d_score, q_sub)
            dv_pair = dv_sub if dv_pair is None else dv_pair + dv_sub
            dk_pair = dk_sub if dk_pair is None else dk_pair + dk_sub
            dq_parts.append(dot(k_tr[sub * 64:(sub + 1) * 64], d_score))
        dqkv[:, base:base + 128] = (jnp.concatenate(dq_parts, axis=0).T * 0.125).astype(BF)
        dqkv[:, d_model + base:d_model + base + 128] = dk_pair.astype(BF)
        dqkv[:, 2 * d_model + base:2 * d_model + base + 128] = dv_pair.astype(BF)

    hid = h_ref[...].astype(F32)
    scale = rms_scale(hid)
    normed = (hid * scale).astype(BF)
    for part in range(3):
        cols = slice(part * d_model, (part + 1) * d_model)
        g_acc[:, cols] += dot(normed, dqkv[:, cols], TN)
    if with_input:
        ct_norm = dot(dqkv[...], w_ref[...], NT).astype(BF).astype(F32)
        ct_h_ref[...] = (ct_mid_ref[...].astype(F32) + rms_pull(hid, scale, ct_norm)).astype(BF)

    @pl.when(step == last)
    def _():
        copy = pltpu.make_async_copy(g_acc, g_out, sem)
        copy.start()
        copy.wait()


def attn_backward(hidden, qkv, lse, ct_attn, ct_mid, w_qkv, with_input):
    seqs, seq_len, d_model = hidden.shape
    heads = d_model // 64
    flops = (4 if with_input else 2) * seqs * seq_len * d_model * 3 * d_model + 20 * seqs * heads * seq_len * seq_len * 128
    row_spec = pl.BlockSpec((None, seq_len, d_model), lambda i: (i, 0, 0))
    in_specs = [row_spec, pl.BlockSpec((None, seq_len, 3 * d_model), lambda i: (i, 0, 0)),
                pl.BlockSpec((None, heads, seq_len), lambda i: (i, 0, 0)), row_spec]
    args = [hidden, qkv, lse, ct_attn]
    out_specs = [pl.BlockSpec(memory_space=pl.ANY)]
    out_shape = [jax.ShapeDtypeStruct((d_model, 3 * d_model), F32)]
    if with_input:
        in_specs += [row_spec, pl.BlockSpec((d_model, 3 * d_model), lambda i: (0, 0), pipeline_mode=pl.Buffered(1))]
        args += [ct_mid, w_qkv]
        out_specs = [row_spec] + out_specs
        out_shape = [jax.ShapeDtypeStruct((seqs, seq_len, d_model), BF)] + out_shape
    return pl.pallas_call(
        functools.partial(attn_bwd_kernel, with_input),
        grid=(seqs,),
        in_specs=in_specs,
        out_specs=out_specs,
        out_shape=out_shape,
        scratch_shapes=[
            pltpu.VMEM((seq_len, 3 * d_model), BF),
            pltpu.VMEM((d_model, 3 * d_model), F32),
            pltpu.SemaphoreType.DMA,
        ],
        cost_estimate=pl.CostEstimate(flops=flops, bytes_accessed=50 << 20, transcendentals=0),
        compiler_params=pltpu.CompilerParams(vmem_limit_bytes=VMEM_LIMIT),
        name='attn_bwd_in' if with_input else 'attn_bwd_first',
    )(*args)


def solution(mesh):
    stages = mesh.shape['pp']
    both = ('dp', 'pp')

    def device_step(act_in, loss_seed, w_qkv, w_proj, w_up, w_down):
        stage = lax.axis_index('pp')
        micro = act_in.shape[0] // stages
        seq_len, d_model = act_in.shape[2:]
        seqs = micro * act_in.shape[1]
        tokens = seqs * seq_len
        parts = (w_qkv.reshape(w_qkv.shape[1], -1), w_proj[0], w_up[0], w_down[0])

        layer_shards = ([], [])
        for part in parts:
            half = part.shape[0] // 2
            kept = lax.dynamic_slice_in_dim(part, stage * half, half, 0)
            sent = lax.dynamic_slice_in_dim(part, (1 - stage) * half, half, 0)
            got = lax.ppermute(sent, 'pp', [(0, 1), (1, 0)])
            layer_shards[0].append(jnp.where(stage == 0, kept, got))
            layer_shards[1].append(jnp.where(stage == 0, got, kept))
        weights = [[lax.all_gather(shard, both, axis=0, tiled=True) for shard in shards] for shards in layer_shards]

        hidden = lax.dynamic_slice_in_dim(act_in, stage * micro, micro, 0).reshape(seqs, seq_len, d_model)
        ct = lax.dynamic_slice_in_dim(loss_seed, stage * micro, micro, 0).reshape(tokens, d_model)

        saved = []
        for layer in range(2):
            wq, wp, wu, wd = weights[layer]
            qkv, attn, lse = attn_forward(hidden, wq)
            attn = attn.reshape(tokens, d_model)
            mid, up, out = mlp_forward(hidden.reshape(tokens, d_model), attn, wp, wu, wd)
            saved.append((hidden, qkv, attn, lse, mid, up))
            hidden = out.reshape(seqs, seq_len, d_model)

        half_len = seq_len // 2
        final = hidden.reshape(micro, act_in.shape[1], seq_len, d_model)
        kept = lax.dynamic_slice_in_dim(final, stage * half_len, half_len, 2)
        sent = lax.dynamic_slice_in_dim(final, (1 - stage) * half_len, half_len, 2)
        got = lax.ppermute(sent, 'pp', [(0, 1), (1, 0)])
        act_out = jnp.where(stage == 0, jnp.concatenate([kept, got]), jnp.concatenate([got, kept]))

        def reduce_rows(grad, layer):
            block = lax.psum_scatter(grad, both, scatter_dimension=0, tiled=True)
            got = lax.ppermute(block, 'pp', [(1 - layer, layer)])
            return jnp.concatenate([block, got] if layer == 0 else [got, block])

        reduced = [None, None]
        for layer in (1, 0):
            wq, wp, wu, wd = weights[layer]
            hid, qkv, attn, lse, mid, up = saved[layer]
            ct_mid, ct_attn, gd, gu, gp = mlp_backward(ct, up, mid, attn, wp, wu, wd)
            shape3 = (seqs, seq_len, d_model)
            res = attn_backward(hid, qkv, lse, ct_attn.reshape(shape3), ct_mid.reshape(shape3), wq, layer > 0)
            gq = res[-1]
            ct = res[0].reshape(tokens, d_model) if layer > 0 else None
            reduced[layer] = [reduce_rows(grad, layer) for grad in (gd, gu, gp, gq)]
        gd, gu, gp, gq = [jnp.where(stage == 0, first, second) for first, second in zip(*reduced)]
        return gq.reshape(w_qkv.shape), gp[None], gu[None], gd[None], act_out

    weight_spec = P('pp', 'dp')
    act_spec = P(None, 'dp')
    return jax.shard_map(device_step, mesh=mesh, in_specs=(act_spec, act_spec, weight_spec, weight_spec, weight_spec, weight_spec), out_specs=(weight_spec, weight_spec, weight_spec, weight_spec, P(None, 'dp', 'pp')), check_vma=False)
```

```python
import functools
import math

import jax
import jax.numpy as jnp
from jax import lax
from jax.experimental import pallas as pl
from jax.experimental.pallas import tpu as pltpu
from jax.sharding import PartitionSpec as P


NORM_EPS = 1e-6
BF = jnp.bfloat16
F32 = jnp.float32
VMEM_LIMIT = 62 * 1024 * 1024
GELU_C = math.sqrt(2.0 / math.pi)
NN = (((1,), (0,)), ((), ()))
NT = (((1,), (1,)), ((), ()))
TN = (((0,), (0,)), ((), ()))


def dot(lhs, rhs, dims=NN):
    return lax.dot_general(lhs, rhs, dims, preferred_element_type=F32)


def rms_scale(hid_f32):
    return lax.rsqrt(jnp.mean(hid_f32 * hid_f32, axis=-1, keepdims=True) + NORM_EPS)


def rms_pull(hid_f32, scale, ct):
    inner = jnp.mean(ct * hid_f32, axis=-1, keepdims=True)
    return scale * (ct - hid_f32 * (scale * scale * inner))


def gelu_parts(pre):
    sq = pre * pre
    th = jnp.tanh(pre * (GELU_C + (GELU_C * 0.044715) * sq))
    half = 0.5 + 0.5 * th
    return sq, th, half


def head_masks(value):
    lane = lax.broadcasted_iota(jnp.int32, (1, 128), 1)
    low = jnp.where(lane < 64, value, 0.0).astype(BF)
    high = jnp.where(lane < 64, 0.0, value).astype(BF)
    return low, high


def causal_tile():
    return lax.broadcasted_iota(jnp.int32, (128, 128), 0) <= lax.broadcasted_iota(jnp.int32, (128, 128), 1)


def attn_fwd_kernel(off_ref, h_ref, w_ref, qkv_ref, attn_ref, lse_ref, held):
    step = pl.program_id(0)
    d_model = h_ref.shape[-1]
    hid = h_ref[...].astype(F32)
    normed = (hid * rms_scale(hid)).astype(BF)
    fresh = lax.rem(step, 2)
    ready = 1 - fresh

    def project(tile):
        cols = slice(tile * 256, (tile + 1) * 256)
        part = dot(normed, w_ref[:, cols]).astype(BF)
        qkv_ref[:, cols] = part
        held[fresh, :, cols] = part

    masks = head_masks(0.125)
    keep = causal_tile()
    zero_tile = jnp.zeros((128, 128), BF)
    heads = d_model // 64

    def score(head):
        base = (head // 2) * 128
        q_pair = held[ready, :, base:base + 128]
        k_pair = held[ready, :, d_model + base:d_model + base + 128]
        return dot(k_pair, q_pair * masks[head % 2], NT)

    tiles = 3 * d_model // 256
    scores = score(0)
    outs = []
    for head in range(heads):
        following = score(head + 1) if head + 1 < heads else None
        for tile in range(head * tiles // heads, (head + 1) * tiles // heads):
            project(tile)
        s00 = jnp.where(keep, scores[:128, :128], -1e30)
        s01 = scores[:128, 128:]
        s11 = jnp.where(keep, scores[128:, 128:], -1e30)
        top0 = jnp.max(s00, axis=0, keepdims=True)
        top1 = jnp.max(jnp.maximum(s01, s11), axis=0, keepdims=True)
        e00 = jnp.exp(s00 - top0)
        e01 = jnp.exp(s01 - top1)
        e11 = jnp.exp(s11 - top1)
        sum0 = jnp.sum(e00, axis=0, keepdims=True)
        sum1 = jnp.sum(e01 + e11, axis=0, keepdims=True)
        inv0 = 1.0 / sum0
        inv1 = 1.0 / sum1
        prob = jnp.concatenate([
            jnp.concatenate([(e00 * inv0).astype(BF), (e01 * inv1).astype(BF)], axis=1),
            jnp.concatenate([zero_tile, (e11 * inv1).astype(BF)], axis=1)], axis=0)
        lse_ref[head:head + 1, :] = jnp.concatenate([top0 + jnp.log(sum0), top1 + jnp.log(sum1)], axis=1)
        base = (head // 2) * 128
        if head % 2 == 0:
            v_tr = held[ready, :, 2 * d_model + base:2 * d_model + base + 128].T
        outs.append(dot(v_tr[(head % 2) * 64:(head % 2 + 1) * 64], prob))
        if head % 2 == 1:
            attn_ref[:, base:base + 128] = jnp.concatenate(outs, axis=0).T.astype(BF)
            outs = []
        scores = following


def attn_forward(offset, hidden, w_qkv, layer, seqs):
    _, seq_len, d_model = hidden.shape
    heads = d_model // 64
    flops = 2 * seqs * seq_len * d_model * 3 * d_model + 8 * seqs * heads * seq_len * seq_len * 128
    now = lambda i: jnp.minimum(i, seqs - 1)
    before = lambda i: jnp.maximum(i - 1, 0)
    return pl.pallas_call(
        attn_fwd_kernel,
        grid_spec=pltpu.PrefetchScalarGridSpec(
            num_scalar_prefetch=1,
            grid=(seqs + 1,),
            in_specs=[
                pl.BlockSpec((None, seq_len, d_model), lambda i, off: (now(i) + off[0] * seqs, 0, 0)),
                pl.BlockSpec((d_model, 3 * d_model), lambda i, off: (layer, 0), pipeline_mode=pl.Buffered(1)),
            ],
            out_specs=[
                pl.BlockSpec((None, seq_len, 3 * d_model), lambda i, off: (now(i), 0, 0)),
                pl.BlockSpec((None, seq_len, d_model), lambda i, off: (before(i), 0, 0)),
                pl.BlockSpec((None, heads, seq_len), lambda i, off: (before(i), 0, 0)),
            ],
            scratch_shapes=[pltpu.VMEM((2, seq_len, 3 * d_model), BF)],
        ),
        out_shape=[
            jax.ShapeDtypeStruct((seqs, seq_len, 3 * d_model), BF),
            jax.ShapeDtypeStruct((seqs, seq_len, d_model), BF),
            jax.ShapeDtypeStruct((seqs, heads, seq_len), F32),
        ],
        cost_estimate=pl.CostEstimate(flops=flops, bytes_accessed=40 << 20, transcendentals=0),
        compiler_params=pltpu.CompilerParams(vmem_limit_bytes=VMEM_LIMIT),
    )(offset, hidden, w_qkv)


def bundle_slices(d_model, d_ff, blocks):
    down, rows, parts = d_ff // blocks, d_model // blocks, d_ff // d_model
    pieces = []
    for blk in range(blocks):
        pieces.append(('proj', blk, pl.ds(down + parts * rows, rows), (pl.ds(blk * rows, rows), slice(None))))
    for part in range(parts):
        for blk in range(blocks):
            pieces.append((('up', part), blk, pl.ds(down + part * rows, rows), (pl.ds(blk * rows, rows), pl.ds(part * d_model, d_model))))
        for sub in range(blocks // parts):
            blk = part * (blocks // parts) + sub
            pieces.append((('down', part), blk, pl.ds(0, down), (pl.ds(blk * down, down), slice(None))))
    return pieces


def bundle_copies(bundle, proj, up, down, sems, to_bundle):
    found = {}
    for idx, (kind, blk, rows, spot) in enumerate(bundle_slices(proj.shape[0], up.shape[1], bundle.shape[0])):
        matrix = proj if kind == 'proj' else (up if kind[0] == 'up' else down)
        ends = (bundle.at[blk, rows, :], matrix.at[spot])
        src, dst = ends[::-1] if to_bundle else ends
        found.setdefault(kind, []).append(pltpu.make_async_copy(src, dst, sems.at[idx]))
    return found


def start_all(copies):
    for copy in copies:
        copy.start()


def wait_all(copies):
    for copy in copies:
        copy.wait()


def mlp_fwd_kernel(chunk, split, off_ref, h_ref, attn_ref, wb_ref, mid_ref, up_ref, *refs):
    out_refs, (wp_ref, wu_ref, wd_ref, sems) = refs[:-4], refs[-4:]
    first = pl.program_id(0) == 0
    loads = bundle_copies(wb_ref, wp_ref, wu_ref, wd_ref, sems, False)

    @pl.when(first)
    def _():
        for copies in loads.values():
            start_all(copies)
        wait_all(loads['proj'])

    mid = (h_ref[...].astype(F32) + dot(attn_ref[...], wp_ref[...])).astype(BF)
    mid_ref[...] = mid
    mid = mid.astype(F32)
    normed = (mid * rms_scale(mid)).astype(BF)
    total = mid

    @pl.when(first)
    def _():
        for kind, copies in loads.items():
            if kind != 'proj':
                wait_all(copies)

    for part in range(wu_ref.shape[1] // chunk):
        cols = slice(part * chunk, (part + 1) * chunk)
        up = dot(normed, wu_ref[:, cols]).astype(BF)
        up_ref[:, cols] = up
        pre = up.astype(F32)
        act = (pre * gelu_parts(pre)[2]).astype(BF)
        total = total + dot(act, wd_ref[cols, :])
    if split:
        own = off_ref[1] == 0
        half = split // 2
        for seq in range(total.shape[0] // split):
            lower = total[seq * split:seq * split + half]
            upper = total[seq * split + half:(seq + 1) * split]
            out_refs[0][seq] = jnp.where(own, lower, upper).astype(BF)
            out_refs[1][seq] = jnp.where(own, upper, lower).astype(BF)
    else:
        out_refs[0][...] = total.astype(BF)


def mlp_forward(offset, hidden, attn, bundle, d_ff, split=0, rows=512, chunk=768):
    tokens, d_model = attn.shape
    steps = tokens // rows
    flops = 2 * tokens * d_model * (d_model + 2 * d_ff)
    row_spec = pl.BlockSpec((rows, d_model), lambda i, off: (i, 0))
    pieces = len(bundle_slices(d_model, d_ff, bundle.shape[0]))
    return pl.pallas_call(
        functools.partial(mlp_fwd_kernel, chunk, split),
        grid_spec=pltpu.PrefetchScalarGridSpec(
            num_scalar_prefetch=1,
            grid=(steps,),
            in_specs=[pl.BlockSpec((rows, d_model), lambda i, off: (i + off[0] * steps, 0)), row_spec, pl.BlockSpec(memory_space=pl.ANY)],
            out_specs=[row_spec, pl.BlockSpec((rows, d_ff), lambda i, off: (i, 0))]
            + ([pl.BlockSpec((rows // split, split // 2, d_model), lambda i, off: (i, 0, 0))] * 2 if split else [row_spec]),
            scratch_shapes=[
                pltpu.VMEM((d_model, d_model), BF),
                pltpu.VMEM((d_model, d_ff), BF),
                pltpu.VMEM((d_ff, d_model), BF),
                pltpu.SemaphoreType.DMA((pieces,)),
            ],
        ),
        out_shape=[
            jax.ShapeDtypeStruct((tokens, d_model), BF),
            jax.ShapeDtypeStruct((tokens, d_ff), BF),
        ] + ([jax.ShapeDtypeStruct((tokens // split, split // 2, d_model), BF)] * 2 if split else [jax.ShapeDtypeStruct((tokens, d_model), BF)]),
        cost_estimate=pl.CostEstimate(flops=flops, bytes_accessed=50 << 20, transcendentals=0),
        compiler_params=pltpu.CompilerParams(vmem_limit_bytes=VMEM_LIMIT),
    )(offset, hidden, attn, bundle)


def mlp_bwd_kernel(chunk, off_ref, ct_ref, up_ref, mid_ref, wb_ref, ct_up_ref, g_out, wd_ref, gu_acc, gd_acc, in_sems, out_sems):
    step = pl.program_id(0)
    first = step == 0
    last = step == pl.num_programs(0) - 1
    d_model = ct_ref.shape[-1]
    blocks = wb_ref.shape[0]
    down = gd_acc.shape[0] // blocks
    rows = d_model // blocks
    ff_parts = gd_acc.shape[0] // d_model
    loads = [pltpu.make_async_copy(wb_ref.at[blk, pl.ds(0, down), :], wd_ref.at[pl.ds(blk * down, down), :], in_sems.at[blk]) for blk in range(blocks)]
    stores = []
    for blk in range(blocks):
        stores.append(pltpu.make_async_copy(gd_acc.at[pl.ds(blk * down, down), :], g_out.at[blk, pl.ds(0, down), :], out_sems.at[len(stores)]))
        for part in range(ff_parts):
            stores.append(pltpu.make_async_copy(gu_acc.at[pl.ds(blk * rows, rows), pl.ds(part * d_model, d_model)],
                                                g_out.at[blk, pl.ds(down + part * rows, rows), :], out_sems.at[len(stores)]))

    @pl.when(first)
    def _():
        start_all(loads)
        gd_acc[...] = jnp.zeros_like(gd_acc)
        gu_acc[...] = jnp.zeros_like(gu_acc)
        wait_all(loads)

    ct = ct_ref[...]
    mid = mid_ref[...].astype(F32)
    normed = (mid * rms_scale(mid)).astype(BF)

    def act_part(part):
        cols = slice(part * chunk, (part + 1) * chunk)
        ct_act = dot(ct, wd_ref[cols, :], NT).astype(BF).astype(F32)
        pre = up_ref[:, cols].astype(F32)
        sq, th, half = gelu_parts(pre)
        act = (pre * half).astype(BF)
        slope = half + (0.5 * pre) * (1.0 - th * th) * (GELU_C + (3.0 * 0.044715 * GELU_C) * sq)
        return act, (ct_act * slope).astype(BF)

    parts = wd_ref.shape[0] // chunk
    now = act_part(0)
    for part in range(parts):
        cols = slice(part * chunk, (part + 1) * chunk)
        act, ct_up = now
        ct_up_ref[:, cols] = ct_up
        now = act_part(part + 1) if part + 1 < parts else None
        gd_acc[cols, :] += dot(act, ct, TN)
        gu_acc[:, cols] += dot(normed, ct_up, TN)

    @pl.when(last)
    def _():
        start_all(stores)
        wait_all(stores)


def mlp_backward(offset, ct, up, mid, bundle, rows=512, chunk=768):
    tokens, d_model = mid.shape
    d_ff = up.shape[1]
    steps = tokens // rows
    blocks = bundle.shape[0]
    row_spec = pl.BlockSpec((rows, d_model), lambda i, off: (i, 0))
    wide_spec = pl.BlockSpec((rows, d_ff), lambda i, off: (i, 0))
    hbm = pl.BlockSpec(memory_space=pl.ANY)
    return pl.pallas_call(
        functools.partial(mlp_bwd_kernel, chunk),
        grid_spec=pltpu.PrefetchScalarGridSpec(
            num_scalar_prefetch=1,
            grid=(steps,),
            in_specs=[pl.BlockSpec((rows, d_model), lambda i, off: (i + off[0] * steps, 0)), wide_spec, row_spec, hbm],
            out_specs=[wide_spec, hbm],
            scratch_shapes=[
                pltpu.VMEM((d_ff, d_model), BF),
                pltpu.VMEM((d_model, d_ff), F32),
                pltpu.VMEM((d_ff, d_model), F32),
                pltpu.SemaphoreType.DMA((blocks,)),
                pltpu.SemaphoreType.DMA((blocks * (1 + d_ff // d_model),)),
            ],
        ),
        out_shape=[
            jax.ShapeDtypeStruct((tokens, d_ff), BF),
            jax.ShapeDtypeStruct((blocks, 2 * d_ff // blocks, d_model), F32),
        ],
        cost_estimate=pl.CostEstimate(flops=6 * tokens * d_model * d_ff, bytes_accessed=70 << 20, transcendentals=0),
        compiler_params=pltpu.CompilerParams(vmem_limit_bytes=VMEM_LIMIT),
    )(offset, ct, up, mid, bundle)


def attn_bwd_kernel(with_input, *refs):
    if with_input:
        off_ref, h_ref, qkv_ref, lse_ref, ct_up_ref, mid_ref, ct_ref, attn_ref, wb_ref, w_ref, ct_h_ref, g_out, ct_attn, dqkv, wp_ref, wu_ref, g_acc, sems = refs
    else:
        off_ref, h_ref, qkv_ref, lse_ref, ct_up_ref, mid_ref, ct_ref, attn_ref, wb_ref, g_out, ct_attn, dqkv, wp_ref, wu_ref, g_acc, sems = refs
    step = pl.program_id(0)
    last = step == pl.num_programs(0) - 1
    d_model = h_ref.shape[-1]
    blocks = wb_ref.shape[0]
    rows = d_model // blocks
    ff_parts = wu_ref.shape[1] // d_model
    down = wb_ref.shape[1] - rows * (1 + ff_parts)
    loads = []
    for blk in range(blocks):
        spot = pl.ds(blk * rows, rows)
        for part in range(ff_parts):
            loads.append(pltpu.make_async_copy(wb_ref.at[blk, pl.ds(down + part * rows, rows), :], wu_ref.at[spot, pl.ds(part * d_model, d_model)], sems.at[len(loads)]))
        loads.append(pltpu.make_async_copy(wb_ref.at[blk, pl.ds(down + ff_parts * rows, rows), :], wp_ref.at[spot, :], sems.at[len(loads)]))

    @pl.when(step == 0)
    def _():
        start_all(loads)
        g_acc[...] = jnp.zeros_like(g_acc)
        wait_all(loads)

    mid = mid_ref[...].astype(F32)
    ct_norm2 = dot(ct_up_ref[...], wu_ref[...], NT).astype(BF).astype(F32)
    ct_mid = (ct_ref[...].astype(F32) + rms_pull(mid, rms_scale(mid), ct_norm2)).astype(BF)
    ct_attn[...] = dot(ct_mid, wp_ref[...], NT).astype(BF)
    g_acc[:, 3 * d_model:] += dot(attn_ref[...], ct_mid, TN)

    q_masks = head_masks(0.125)
    o_masks = head_masks(1.0)
    keep = causal_tile()
    zero_tile = jnp.zeros((128, 128), BF)

    def square(t00, t01, t11):
        return jnp.concatenate([
            jnp.concatenate([t00.astype(BF), t01.astype(BF)], axis=1),
            jnp.concatenate([zero_tile, t11.astype(BF)], axis=1)], axis=0)

    def begin(head):
        base = (head // 2) * 128
        k_pair = qkv_ref[:, d_model + base:d_model + base + 128]
        v_pair = qkv_ref[:, 2 * d_model + base:2 * d_model + base + 128]
        q_sub = qkv_ref[:, base:base + 128] * q_masks[head % 2]
        o_sub = ct_attn[:, base:base + 128] * o_masks[head % 2]
        return q_sub, o_sub, dot(k_pair, q_sub, NT), dot(v_pair, o_sub, NT)

    heads = d_model // 64
    now = begin(0)
    for head in range(heads):
        following = begin(head + 1) if head + 1 < heads else None
        base = (head // 2) * 128
        q_sub, o_sub, scores, d_prob = now
        if head % 2 == 0:
            k_tr = qkv_ref[:, d_model + base:d_model + base + 128].T
            dq_parts = []
        lse0 = lse_ref[head:head + 1, :128]
        lse1 = lse_ref[head:head + 1, 128:]
        p00 = jnp.exp(jnp.where(keep, scores[:128, :128] - lse0, -1e30))
        p01 = jnp.exp(scores[:128, 128:] - lse1)
        p11 = jnp.exp(jnp.where(keep, scores[128:, 128:] - lse1, -1e30))
        d00 = d_prob[:128, :128].astype(BF).astype(F32)
        d01 = d_prob[:128, 128:].astype(BF).astype(F32)
        d11 = d_prob[128:, 128:].astype(BF).astype(F32)
        m0 = jnp.sum(p00 * d00, axis=0, keepdims=True)
        m1 = jnp.sum(p01 * d01 + p11 * d11, axis=0, keepdims=True)
        d_score = square(p00 * (d00 - m0), p01 * (d01 - m1), p11 * (d11 - m1))
        dv_sub = dot(square(p00, p01, p11), o_sub)
        dk_sub = dot(d_score, q_sub)
        dq_parts.append(dot(k_tr[(head % 2) * 64:(head % 2 + 1) * 64], d_score))
        if head % 2 == 0:
            dv_pair, dk_pair = dv_sub, dk_sub
        else:
            dqkv[:, base:base + 128] = (jnp.concatenate(dq_parts, axis=0).T * 0.125).astype(BF)
            dqkv[:, d_model + base:d_model + base + 128] = (dk_pair + dk_sub).astype(BF)
            dqkv[:, 2 * d_model + base:2 * d_model + base + 128] = (dv_pair + dv_sub).astype(BF)
        now = following

    hid = h_ref[...].astype(F32)
    scale = rms_scale(hid)
    normed = (hid * scale).astype(BF)
    for part in range(3):
        cols = slice(part * d_model, (part + 1) * d_model)
        g_acc[:, cols] += dot(normed, dqkv[:, cols], TN)
    if with_input:
        ct_norm = dot(dqkv[...], w_ref[...], NT).astype(BF).astype(F32)
        ct_h_ref[...] = (ct_mid.astype(F32) + rms_pull(hid, scale, ct_norm)).astype(BF)

    @pl.when(last)
    def _():
        copy = pltpu.make_async_copy(g_acc, g_out, sems.at[len(loads)])
        copy.start()
        copy.wait()


def attn_backward(offsets, hidden, qkv, lse, ct_up, mid, ct, attn, bundle, w_qkv, with_input):
    seqs, seq_len = qkv.shape[:2]
    d_model, d_ff = hidden.shape[-1], ct_up.shape[-1]
    heads = d_model // 64
    blocks = bundle.shape[0]
    flops = 2 * seqs * seq_len * d_model * (d_ff + d_model * (8 if with_input else 5)) + 20 * seqs * heads * seq_len * seq_len * 128
    block = lambda width, which=None: pl.BlockSpec((None, seq_len, width), (lambda i, off: (i, 0, 0)) if which is None else (lambda i, off: (i + off[which] * seqs, 0, 0)))
    hbm = pl.BlockSpec(memory_space=pl.ANY)
    in_specs = [block(d_model, 0), block(3 * d_model), pl.BlockSpec((None, heads, seq_len), lambda i, off: (i, 0, 0)),
                block(d_ff), block(d_model), block(d_model, 1), block(d_model), hbm]
    args = [offsets, hidden, qkv, lse, ct_up, mid, ct, attn, bundle]
    out_specs = [hbm]
    out_shape = [jax.ShapeDtypeStruct((d_model, 4 * d_model), F32)]
    if with_input:
        in_specs.append(pl.BlockSpec((d_model, 3 * d_model), lambda i, off: (1, 0), pipeline_mode=pl.Buffered(1)))
        args.append(w_qkv)
        out_specs = [block(d_model)] + out_specs
        out_shape = [jax.ShapeDtypeStruct((seqs, seq_len, d_model), BF)] + out_shape
    return pl.pallas_call(
        functools.partial(attn_bwd_kernel, with_input),
        grid_spec=pltpu.PrefetchScalarGridSpec(
            num_scalar_prefetch=1,
            grid=(seqs,),
            in_specs=in_specs,
            out_specs=out_specs,
            scratch_shapes=[
                pltpu.VMEM((seq_len, d_model), BF),
                pltpu.VMEM((seq_len, 3 * d_model), BF),
                pltpu.VMEM((d_model, d_model), BF),
                pltpu.VMEM((d_model, d_ff), BF),
                pltpu.VMEM((d_model, 4 * d_model), F32),
                pltpu.SemaphoreType.DMA((blocks * (1 + d_ff // d_model) + 1,)),
            ],
        ),
        out_shape=out_shape,
        cost_estimate=pl.CostEstimate(flops=flops, bytes_accessed=50 << 20, transcendentals=0),
        compiler_params=pltpu.CompilerParams(vmem_limit_bytes=VMEM_LIMIT),
    )(*args)


def solution(mesh):
    stages = mesh.shape['pp']
    both = ('dp', 'pp')
    swap = [(0, 1), (1, 0)]

    def device_step(act_in, loss_seed, w_qkv, w_proj, w_up, w_down):
        stage = lax.axis_index('pp')
        micro = act_in.shape[0] // stages
        seq_len, d_model = act_in.shape[2:]
        d_ff = w_up.shape[2]
        ff_parts = d_ff // d_model
        seqs = micro * act_in.shape[1]
        tokens = seqs * seq_len
        own = stage.astype(jnp.int32).reshape(1)
        zero = jnp.zeros((1,), jnp.int32)

        wq_shard = w_qkv.reshape(-1, 3 * d_model)
        wq = lax.all_gather(wq_shard, ('pp', 'dp'), axis=0, tiled=True)
        w_proj, w_up, w_down, _ = lax.optimization_barrier((w_proj, w_up, w_down, wq_shard))

        rows = w_proj.shape[1] // 2
        mlp_halves = jnp.concatenate(
            [w_down[0].reshape(2, -1, d_model)]
            + [w_up[0, :, part * d_model:(part + 1) * d_model].reshape(2, rows, d_model) for part in range(ff_parts)]
            + [w_proj[0].reshape(2, rows, d_model)], axis=1)
        kept = lax.dynamic_index_in_dim(mlp_halves, stage, 0, keepdims=False)
        got = lax.ppermute(lax.dynamic_index_in_dim(mlp_halves, 1 - stage, 0, keepdims=False), 'pp', swap)
        bundles = []
        for layer in range(2):
            bundles.append(lax.all_gather(jnp.where(stage == layer, kept, got), both, axis=0))

        hidden = act_in.reshape(stages * seqs, seq_len, d_model)
        saved = []
        for layer in range(2):
            off = own if layer == 0 else zero
            wb = bundles[layer]
            qkv, attn, lse = attn_forward(off, hidden, wq, layer, seqs)
            attn = attn.reshape(tokens, d_model)
            offs = jnp.concatenate([off, own])
            mid, up, *outs = mlp_forward(offs, hidden.reshape(-1, d_model), attn, wb, d_ff, split=seq_len if layer == 1 else 0)
            saved.append((hidden, qkv, attn, lse, mid, up))
            hidden = outs[0].reshape(seqs, -1, d_model)
        half_shape = (micro, act_in.shape[1], seq_len // 2, d_model)
        final_kept, final_sent = [out.reshape(half_shape) for out in outs]
        final_got = lax.ppermute(final_sent, 'pp', swap)
        act_out = jnp.where(stage == 0, jnp.concatenate([final_kept, final_got]), jnp.concatenate([final_got, final_kept]))

        def reduce_rows(grad, layer):
            block = lax.psum_scatter(grad, both, scatter_dimension=0, tiled=True)
            got = lax.ppermute(block, 'pp', [(1 - layer, layer)])
            return (block, got) if layer == 0 else (got, block)

        def reduce_stage(grad, layer):
            block = lax.psum_scatter(grad, 'dp', scatter_dimension=0, tiled=True)
            got = lax.ppermute(block, 'pp', [(1 - layer, layer)])
            return block, got

        ct = loss_seed.reshape(stages * tokens, d_model)
        shape3 = (-1, seq_len, d_model)
        reduced = [None, None]
        for layer in (1, 0):
            wb = bundles[layer]
            hid, qkv, attn, lse, mid, up = saved[layer]
            ct_up, g_mlp = mlp_backward(own if layer == 1 else zero, ct, up, mid, wb)
            if layer == 0:
                ct_up, act_out = lax.optimization_barrier((ct_up, act_out))
            mlp_part = reduce_rows(g_mlp, layer)
            offsets = jnp.concatenate([zero, own] if layer == 1 else [own, zero])
            res = attn_backward(offsets, hid, qkv, lse, ct_up.reshape(seqs, seq_len, d_ff), mid.reshape(shape3), ct.reshape(shape3), attn.reshape(shape3),
                                wb, wq, layer > 0)
            attn_part = reduce_stage(res[-1], layer)
            reduced[layer] = (mlp_part, attn_part)
            if layer == 1:
                ct = res[0].reshape(tokens, d_model)
        pick = lambda first, second: jnp.where(stage == 0, first, second)
        mlp = [pick(reduced[0][0][half], reduced[1][0][half]).reshape(-1, d_model) for half in range(2)]
        wide = pick(*[sum(reduced[layer][1]) for layer in range(2)])
        down = d_ff // (2 * mesh.shape['dp'])
        gd = jnp.concatenate([half[:down] for half in mlp])
        gu = jnp.concatenate([jnp.concatenate([half[down + part * rows:down + (part + 1) * rows] for part in range(ff_parts)], axis=1) for half in mlp])
        gq, gp = wide[:, :3 * d_model], wide[:, 3 * d_model:]
        return gq.reshape(w_qkv.shape), gp[None], gu[None], gd[None], act_out

    weight_spec = P('pp', 'dp')
    act_spec = P(None, 'dp')
    return jax.shard_map(device_step, mesh=mesh, in_specs=(act_spec, act_spec, weight_spec, weight_spec, weight_spec, weight_spec), out_specs=(weight_spec, weight_spec, weight_spec, weight_spec, P(None, 'dp', 'pp')), check_vma=False)
```

```python
import functools
import math

import jax
import jax.numpy as jnp
from jax import lax
from jax.experimental import pallas as pl
from jax.experimental.pallas import tpu as pltpu
from jax.sharding import PartitionSpec as P


NORM_EPS = 1e-6
BF = jnp.bfloat16
F32 = jnp.float32
VMEM_LIMIT = 62 * 1024 * 1024
GELU_C = math.sqrt(2.0 / math.pi)
NN = (((1,), (0,)), ((), ()))
NT = (((1,), (1,)), ((), ()))
TN = (((0,), (0,)), ((), ()))


def dot(lhs, rhs, dims=NN):
    return lax.dot_general(lhs, rhs, dims, preferred_element_type=F32)


def rms_scale(hid_f32):
    return lax.rsqrt(jnp.mean(hid_f32 * hid_f32, axis=-1, keepdims=True) + NORM_EPS)


def rms_pull(hid_f32, scale, ct):
    inner = jnp.mean(ct * hid_f32, axis=-1, keepdims=True)
    return scale * (ct - hid_f32 * (scale * scale * inner))


def gelu_parts(pre):
    sq = pre * pre
    th = jnp.tanh(pre * (GELU_C + (GELU_C * 0.044715) * sq))
    half = 0.5 + 0.5 * th
    return sq, th, half


def head_masks(value):
    lane = lax.broadcasted_iota(jnp.int32, (1, 128), 1)
    low = jnp.where(lane < 64, value, 0.0).astype(BF)
    high = jnp.where(lane < 64, 0.0, value).astype(BF)
    return low, high


def causal_tile():
    return lax.broadcasted_iota(jnp.int32, (128, 128), 0) <= lax.broadcasted_iota(jnp.int32, (128, 128), 1)


def attn_fwd_kernel(off_ref, h_ref, w_ref, qkv_ref, attn_ref, lse_ref, held):
    step = pl.program_id(0)
    d_model = h_ref.shape[-1]
    hid = h_ref[...].astype(F32)
    normed = (hid * rms_scale(hid)).astype(BF)
    fresh = lax.rem(step, 2)
    ready = 1 - fresh

    def project(tile):
        cols = slice(tile * 256, (tile + 1) * 256)
        part = dot(normed, w_ref[:, cols]).astype(BF)
        qkv_ref[:, cols] = part
        held[fresh, :, cols] = part

    masks = head_masks(0.125)
    keep = causal_tile()
    zero_tile = jnp.zeros((128, 128), BF)
    heads = d_model // 64

    def score(head):
        base = (head // 2) * 128
        q_pair = held[ready, :, base:base + 128]
        k_pair = held[ready, :, d_model + base:d_model + base + 128]
        return dot(k_pair, q_pair * masks[head % 2], NT)

    tiles = 3 * d_model // 256
    scores = score(0)
    outs = []
    for head in range(heads):
        following = score(head + 1) if head + 1 < heads else None
        for tile in range(head * tiles // heads, (head + 1) * tiles // heads):
            project(tile)
        s00 = jnp.where(keep, scores[:128, :128], -1e30)
        s01 = scores[:128, 128:]
        s11 = jnp.where(keep, scores[128:, 128:], -1e30)
        top0 = jnp.max(s00, axis=0, keepdims=True)
        top1 = jnp.max(jnp.maximum(s01, s11), axis=0, keepdims=True)
        e00 = jnp.exp(s00 - top0)
        e01 = jnp.exp(s01 - top1)
        e11 = jnp.exp(s11 - top1)
        sum0 = jnp.sum(e00, axis=0, keepdims=True)
        sum1 = jnp.sum(e01 + e11, axis=0, keepdims=True)
        inv0 = 1.0 / sum0
        inv1 = 1.0 / sum1
        prob = jnp.concatenate([
            jnp.concatenate([(e00 * inv0).astype(BF), (e01 * inv1).astype(BF)], axis=1),
            jnp.concatenate([zero_tile, (e11 * inv1).astype(BF)], axis=1)], axis=0)
        lse_ref[head:head + 1, :] = jnp.concatenate([top0 + jnp.log(sum0), top1 + jnp.log(sum1)], axis=1)
        base = (head // 2) * 128
        if head % 2 == 0:
            v_tr = held[ready, :, 2 * d_model + base:2 * d_model + base + 128].T
        outs.append(dot(v_tr[(head % 2) * 64:(head % 2 + 1) * 64], prob))
        if head % 2 == 1:
            attn_ref[:, base:base + 128] = jnp.concatenate(outs, axis=0).T.astype(BF)
            outs = []
        scores = following


def attn_forward(offset, hidden, w_qkv, layer, seqs):
    _, seq_len, d_model = hidden.shape
    heads = d_model // 64
    flops = 2 * seqs * seq_len * d_model * 3 * d_model + 8 * seqs * heads * seq_len * seq_len * 128
    now = lambda i: jnp.minimum(i, seqs - 1)
    before = lambda i: jnp.maximum(i - 1, 0)
    return pl.pallas_call(
        attn_fwd_kernel,
        grid_spec=pltpu.PrefetchScalarGridSpec(
            num_scalar_prefetch=1,
            grid=(seqs + 1,),
            in_specs=[
                pl.BlockSpec((None, seq_len, d_model), lambda i, off: (now(i) + off[0] * seqs, 0, 0)),
                pl.BlockSpec((d_model, 3 * d_model), lambda i, off: (layer, 0), pipeline_mode=pl.Buffered(1)),
            ],
            out_specs=[
                pl.BlockSpec((None, seq_len, 3 * d_model), lambda i, off: (now(i), 0, 0)),
                pl.BlockSpec((None, seq_len, d_model), lambda i, off: (before(i), 0, 0)),
                pl.BlockSpec((None, heads, seq_len), lambda i, off: (before(i), 0, 0)),
            ],
            scratch_shapes=[pltpu.VMEM((2, seq_len, 3 * d_model), BF)],
        ),
        out_shape=[
            jax.ShapeDtypeStruct((seqs, seq_len, 3 * d_model), BF),
            jax.ShapeDtypeStruct((seqs, seq_len, d_model), BF),
            jax.ShapeDtypeStruct((seqs, heads, seq_len), F32),
        ],
        cost_estimate=pl.CostEstimate(flops=flops, bytes_accessed=40 << 20, transcendentals=0),
        compiler_params=pltpu.CompilerParams(vmem_limit_bytes=VMEM_LIMIT),
    )(offset, hidden, w_qkv)


def bundle_slices(d_model, d_ff, blocks):
    down, rows, parts = d_ff // blocks, d_model // blocks, d_ff // d_model
    pieces = []
    for blk in range(blocks):
        pieces.append(('proj', blk, pl.ds(down + parts * rows, rows), (pl.ds(blk * rows, rows), slice(None))))
    for part in range(parts):
        for blk in range(blocks):
            pieces.append((('up', part), blk, pl.ds(down + part * rows, rows), (pl.ds(blk * rows, rows), pl.ds(part * d_model, d_model))))
        for sub in range(blocks // parts):
            blk = part * (blocks // parts) + sub
            pieces.append((('down', part), blk, pl.ds(0, down), (pl.ds(blk * down, down), slice(None))))
    return pieces


def bundle_copies(bundle, proj, up, down, sems, to_bundle):
    found = {}
    for idx, (kind, blk, rows, spot) in enumerate(bundle_slices(proj.shape[0], up.shape[1], bundle.shape[0])):
        matrix = proj if kind == 'proj' else (up if kind[0] == 'up' else down)
        ends = (bundle.at[blk, rows, :], matrix.at[spot])
        src, dst = ends[::-1] if to_bundle else ends
        found.setdefault(kind, []).append(pltpu.make_async_copy(src, dst, sems.at[idx]))
    return found


def start_all(copies):
    for copy in copies:
        copy.start()


def wait_all(copies):
    for copy in copies:
        copy.wait()


def mlp_fwd_kernel(chunk, off_ref, h_ref, attn_ref, wb_ref, mid_ref, up_ref, out_ref, wp_ref, wu_ref, wd_ref, sems):
    first = pl.program_id(0) == 0
    loads = bundle_copies(wb_ref, wp_ref, wu_ref, wd_ref, sems, False)

    @pl.when(first)
    def _():
        for copies in loads.values():
            start_all(copies)
        wait_all(loads['proj'])

    mid = (h_ref[...].astype(F32) + dot(attn_ref[...], wp_ref[...])).astype(BF)
    mid_ref[...] = mid
    mid = mid.astype(F32)
    normed = (mid * rms_scale(mid)).astype(BF)
    total = mid

    @pl.when(first)
    def _():
        for kind, copies in loads.items():
            if kind != 'proj':
                wait_all(copies)

    for part in range(wu_ref.shape[1] // chunk):
        cols = slice(part * chunk, (part + 1) * chunk)
        up = dot(normed, wu_ref[:, cols]).astype(BF)
        up_ref[:, cols] = up
        pre = up.astype(F32)
        act = (pre * gelu_parts(pre)[2]).astype(BF)
        total = total + dot(act, wd_ref[cols, :])
    out_ref[...] = total.astype(BF)


def mlp_forward(offset, hidden, attn, bundle, d_ff, rows=512, chunk=768):
    tokens, d_model = attn.shape
    steps = tokens // rows
    flops = 2 * tokens * d_model * (d_model + 2 * d_ff)
    row_spec = pl.BlockSpec((rows, d_model), lambda i, off: (i, 0))
    pieces = len(bundle_slices(d_model, d_ff, bundle.shape[0]))
    return pl.pallas_call(
        functools.partial(mlp_fwd_kernel, chunk),
        grid_spec=pltpu.PrefetchScalarGridSpec(
            num_scalar_prefetch=1,
            grid=(steps,),
            in_specs=[pl.BlockSpec((rows, d_model), lambda i, off: (i + off[0] * steps, 0)), row_spec, pl.BlockSpec(memory_space=pl.ANY)],
            out_specs=[row_spec, pl.BlockSpec((rows, d_ff), lambda i, off: (i, 0)), row_spec],
            scratch_shapes=[
                pltpu.VMEM((d_model, d_model), BF),
                pltpu.VMEM((d_model, d_ff), BF),
                pltpu.VMEM((d_ff, d_model), BF),
                pltpu.SemaphoreType.DMA((pieces,)),
            ],
        ),
        out_shape=[
            jax.ShapeDtypeStruct((tokens, d_model), BF),
            jax.ShapeDtypeStruct((tokens, d_ff), BF),
            jax.ShapeDtypeStruct((tokens, d_model), BF),
        ],
        cost_estimate=pl.CostEstimate(flops=flops, bytes_accessed=50 << 20, transcendentals=0),
        compiler_params=pltpu.CompilerParams(vmem_limit_bytes=VMEM_LIMIT),
    )(offset, hidden, attn, bundle)


def grad_copies(gu_acc, gd_acc, g_out, sems):
    blocks = g_out.shape[0]
    d_model = g_out.shape[2]
    down = gd_acc.shape[0] // blocks
    rows = d_model // blocks
    stores = []
    for blk in range(blocks):
        stores.append(pltpu.make_async_copy(gd_acc.at[pl.ds(blk * down, down), :], g_out.at[blk, pl.ds(0, down), :], sems.at[len(stores)]))
        for part in range(gd_acc.shape[0] // d_model):
            stores.append(pltpu.make_async_copy(gu_acc.at[pl.ds(blk * rows, rows), pl.ds(part * d_model, d_model)],
                                                g_out.at[blk, pl.ds(down + part * rows, rows), :], sems.at[len(stores)]))
    return stores


def mlp_last_kernel(chunk, half, off_ref, h_ref, attn_ref, ct_ref, wb_ref, mid_ref, ct_up_ref, kept_ref, sent_ref, g_out,
                    wp_ref, wu_ref, wd_ref, gu_acc, gd_acc, in_sems, out_sems):
    step = pl.program_id(0)
    loads = bundle_copies(wb_ref, wp_ref, wu_ref, wd_ref, in_sems, False)
    stores = grad_copies(gu_acc, gd_acc, g_out, out_sems)

    @pl.when(step == 0)
    def _():
        for copies in loads.values():
            start_all(copies)
        gd_acc[...] = jnp.zeros_like(gd_acc)
        gu_acc[...] = jnp.zeros_like(gu_acc)
        for copies in loads.values():
            wait_all(copies)

    ct = ct_ref[...]
    mid = (h_ref[...].astype(F32) + dot(attn_ref[...], wp_ref[...])).astype(BF)
    mid_ref[...] = mid
    mid = mid.astype(F32)
    normed = (mid * rms_scale(mid)).astype(BF)
    total = mid

    def act_part(part):
        cols = slice(part * chunk, (part + 1) * chunk)
        pre = dot(normed, wu_ref[:, cols]).astype(BF).astype(F32)
        ct_act = dot(ct, wd_ref[cols, :], NT).astype(BF).astype(F32)
        sq, th, half_th = gelu_parts(pre)
        act = (pre * half_th).astype(BF)
        slope = half_th + (0.5 * pre) * (1.0 - th * th) * (GELU_C + (3.0 * 0.044715 * GELU_C) * sq)
        return act, (ct_act * slope).astype(BF)

    parts = wd_ref.shape[0] // chunk
    now = act_part(0)
    for part in range(parts):
        cols = slice(part * chunk, (part + 1) * chunk)
        act, ct_up = now
        ct_up_ref[:, cols] = ct_up
        now = act_part(part + 1) if part + 1 < parts else None
        gd_acc[cols, :] += dot(act, ct, TN)
        gu_acc[:, cols] += dot(normed, ct_up, TN)
        total = total + dot(act, wd_ref[cols, :])

    own = off_ref[0] == 0
    for seq in range(kept_ref.shape[0]):
        lower = total[2 * seq * half:(2 * seq + 1) * half]
        upper = total[(2 * seq + 1) * half:(2 * seq + 2) * half]
        kept_ref[seq] = jnp.where(own, lower, upper).astype(BF)
        sent_ref[seq] = jnp.where(own, upper, lower).astype(BF)

    @pl.when(step == pl.num_programs(0) - 1)
    def _():
        start_all(stores)
        wait_all(stores)


def mlp_last(offset, hidden, attn, ct, bundle, d_ff, seq_len, rows=512, chunk=512):
    tokens, d_model = attn.shape
    steps = tokens // rows
    blocks = bundle.shape[0]
    half = seq_len // 2
    row_spec = pl.BlockSpec((rows, d_model), lambda i, off: (i, 0))
    wide_spec = pl.BlockSpec((rows, d_ff), lambda i, off: (i, 0))
    half_spec = pl.BlockSpec((rows // seq_len, half, d_model), lambda i, off: (i, 0, 0))
    hbm = pl.BlockSpec(memory_space=pl.ANY)
    return pl.pallas_call(
        functools.partial(mlp_last_kernel, chunk, half),
        grid_spec=pltpu.PrefetchScalarGridSpec(
            num_scalar_prefetch=1,
            grid=(steps,),
            in_specs=[row_spec, row_spec, pl.BlockSpec((rows, d_model), lambda i, off: (i + off[0] * steps, 0)), hbm],
            out_specs=[row_spec, wide_spec, half_spec, half_spec, hbm],
            scratch_shapes=[
                pltpu.VMEM((d_model, d_model), BF),
                pltpu.VMEM((d_model, d_ff), BF),
                pltpu.VMEM((d_ff, d_model), BF),
                pltpu.VMEM((d_model, d_ff), F32),
                pltpu.VMEM((d_ff, d_model), F32),
                pltpu.SemaphoreType.DMA((len(bundle_slices(d_model, d_ff, blocks)),)),
                pltpu.SemaphoreType.DMA((blocks * (1 + d_ff // d_model),)),
            ],
        ),
        out_shape=[
            jax.ShapeDtypeStruct((tokens, d_model), BF),
            jax.ShapeDtypeStruct((tokens, d_ff), BF),
            jax.ShapeDtypeStruct((tokens // seq_len, half, d_model), BF),
            jax.ShapeDtypeStruct((tokens // seq_len, half, d_model), BF),
            jax.ShapeDtypeStruct((blocks, 2 * d_ff // blocks, d_model), F32),
        ],
        cost_estimate=pl.CostEstimate(flops=2 * tokens * d_model * (d_model + 5 * d_ff), bytes_accessed=70 << 20, transcendentals=0),
        compiler_params=pltpu.CompilerParams(vmem_limit_bytes=VMEM_LIMIT),
    )(offset, hidden, attn, ct, bundle)


def mlp_bwd_kernel(chunk, off_ref, ct_ref, up_ref, mid_ref, wb_ref, ct_up_ref, g_out, wd_ref, gu_acc, gd_acc, in_sems, out_sems):
    step = pl.program_id(0)
    first = step == 0
    last = step == pl.num_programs(0) - 1
    blocks = wb_ref.shape[0]
    down = gd_acc.shape[0] // blocks
    loads = [pltpu.make_async_copy(wb_ref.at[blk, pl.ds(0, down), :], wd_ref.at[pl.ds(blk * down, down), :], in_sems.at[blk]) for blk in range(blocks)]
    stores = grad_copies(gu_acc, gd_acc, g_out, out_sems)

    @pl.when(first)
    def _():
        start_all(loads)
        gd_acc[...] = jnp.zeros_like(gd_acc)
        gu_acc[...] = jnp.zeros_like(gu_acc)
        wait_all(loads)

    ct = ct_ref[...]
    mid = mid_ref[...].astype(F32)
    normed = (mid * rms_scale(mid)).astype(BF)

    def act_part(part):
        cols = slice(part * chunk, (part + 1) * chunk)
        ct_act = dot(ct, wd_ref[cols, :], NT).astype(BF).astype(F32)
        pre = up_ref[:, cols].astype(F32)
        sq, th, half = gelu_parts(pre)
        act = (pre * half).astype(BF)
        slope = half + (0.5 * pre) * (1.0 - th * th) * (GELU_C + (3.0 * 0.044715 * GELU_C) * sq)
        return act, (ct_act * slope).astype(BF)

    parts = wd_ref.shape[0] // chunk
    now = act_part(0)
    for part in range(parts):
        cols = slice(part * chunk, (part + 1) * chunk)
        act, ct_up = now
        ct_up_ref[:, cols] = ct_up
        now = act_part(part + 1) if part + 1 < parts else None
        gd_acc[cols, :] += dot(act, ct, TN)
        gu_acc[:, cols] += dot(normed, ct_up, TN)

    @pl.when(last)
    def _():
        start_all(stores)
        wait_all(stores)


def mlp_backward(offset, ct, up, mid, bundle, rows=256, chunk=768):
    tokens, d_model = mid.shape
    d_ff = up.shape[1]
    steps = tokens // rows
    blocks = bundle.shape[0]
    row_spec = pl.BlockSpec((rows, d_model), lambda i, off: (i, 0))
    wide_spec = pl.BlockSpec((rows, d_ff), lambda i, off: (i, 0))
    hbm = pl.BlockSpec(memory_space=pl.ANY)
    return pl.pallas_call(
        functools.partial(mlp_bwd_kernel, chunk),
        grid_spec=pltpu.PrefetchScalarGridSpec(
            num_scalar_prefetch=1,
            grid=(steps,),
            in_specs=[pl.BlockSpec((rows, d_model), lambda i, off: (i + off[0] * steps, 0)), wide_spec, row_spec, hbm],
            out_specs=[wide_spec, hbm],
            scratch_shapes=[
                pltpu.VMEM((d_ff, d_model), BF),
                pltpu.VMEM((d_model, d_ff), F32),
                pltpu.VMEM((d_ff, d_model), F32),
                pltpu.SemaphoreType.DMA((blocks,)),
                pltpu.SemaphoreType.DMA((blocks * (1 + d_ff // d_model),)),
            ],
        ),
        out_shape=[
            jax.ShapeDtypeStruct((tokens, d_ff), BF),
            jax.ShapeDtypeStruct((blocks, 2 * d_ff // blocks, d_model), F32),
        ],
        cost_estimate=pl.CostEstimate(flops=6 * tokens * d_model * d_ff, bytes_accessed=70 << 20, transcendentals=0),
        compiler_params=pltpu.CompilerParams(vmem_limit_bytes=VMEM_LIMIT),
    )(offset, ct, up, mid, bundle)


def attn_bwd_kernel(with_input, *refs):
    if with_input:
        off_ref, h_ref, qkv_ref, lse_ref, ct_up_ref, mid_ref, ct_ref, attn_ref, wb_ref, w_ref, ct_h_ref, g_out, ct_attn, dqkv, wp_ref, wu_ref, g_acc, sems = refs
    else:
        off_ref, h_ref, qkv_ref, lse_ref, ct_up_ref, mid_ref, ct_ref, attn_ref, wb_ref, g_out, ct_attn, dqkv, wp_ref, wu_ref, g_acc, sems = refs
    step = pl.program_id(0)
    last = step == pl.num_programs(0) - 1
    d_model = h_ref.shape[-1]
    blocks = wb_ref.shape[0]
    rows = d_model // blocks
    ff_parts = wu_ref.shape[1] // d_model
    down = wb_ref.shape[1] - rows * (1 + ff_parts)
    loads = []
    for blk in range(blocks):
        spot = pl.ds(blk * rows, rows)
        for part in range(ff_parts):
            loads.append(pltpu.make_async_copy(wb_ref.at[blk, pl.ds(down + part * rows, rows), :], wu_ref.at[spot, pl.ds(part * d_model, d_model)], sems.at[len(loads)]))
        loads.append(pltpu.make_async_copy(wb_ref.at[blk, pl.ds(down + ff_parts * rows, rows), :], wp_ref.at[spot, :], sems.at[len(loads)]))

    @pl.when(step == 0)
    def _():
        start_all(loads)
        g_acc[...] = jnp.zeros_like(g_acc)
        wait_all(loads)

    mid = mid_ref[...].astype(F32)
    ct_norm2 = dot(ct_up_ref[...], wu_ref[...], NT).astype(BF).astype(F32)
    ct_mid = (ct_ref[...].astype(F32) + rms_pull(mid, rms_scale(mid), ct_norm2)).astype(BF)
    ct_attn[...] = dot(ct_mid, wp_ref[...], NT).astype(BF)
    g_acc[:, 3 * d_model:] += dot(attn_ref[...], ct_mid, TN)

    q_masks = head_masks(0.125)
    o_masks = head_masks(1.0)
    keep = causal_tile()
    zero_tile = jnp.zeros((128, 128), BF)

    def square(t00, t01, t11):
        return jnp.concatenate([
            jnp.concatenate([t00.astype(BF), t01.astype(BF)], axis=1),
            jnp.concatenate([zero_tile, t11.astype(BF)], axis=1)], axis=0)

    def begin(head):
        base = (head // 2) * 128
        k_pair = qkv_ref[:, d_model + base:d_model + base + 128]
        v_pair = qkv_ref[:, 2 * d_model + base:2 * d_model + base + 128]
        q_sub = qkv_ref[:, base:base + 128] * q_masks[head % 2]
        o_sub = ct_attn[:, base:base + 128] * o_masks[head % 2]
        return q_sub, o_sub, dot(k_pair, q_sub, NT), dot(v_pair, o_sub, NT)

    heads = d_model // 64
    now = begin(0)
    for head in range(heads):
        following = begin(head + 1) if head + 1 < heads else None
        base = (head // 2) * 128
        q_sub, o_sub, scores, d_prob = now
        if head % 2 == 0:
            k_tr = qkv_ref[:, d_model + base:d_model + base + 128].T
            dq_parts = []
        lse0 = lse_ref[head:head + 1, :128]
        lse1 = lse_ref[head:head + 1, 128:]
        p00 = jnp.exp(jnp.where(keep, scores[:128, :128] - lse0, -1e30))
        p01 = jnp.exp(scores[:128, 128:] - lse1)
        p11 = jnp.exp(jnp.where(keep, scores[128:, 128:] - lse1, -1e30))
        d00 = d_prob[:128, :128].astype(BF).astype(F32)
        d01 = d_prob[:128, 128:].astype(BF).astype(F32)
        d11 = d_prob[128:, 128:].astype(BF).astype(F32)
        m0 = jnp.sum(p00 * d00, axis=0, keepdims=True)
        m1 = jnp.sum(p01 * d01 + p11 * d11, axis=0, keepdims=True)
        d_score = square(p00 * (d00 - m0), p01 * (d01 - m1), p11 * (d11 - m1))
        dv_sub = dot(square(p00, p01, p11), o_sub)
        dk_sub = dot(d_score, q_sub)
        dq_parts.append(dot(k_tr[(head % 2) * 64:(head % 2 + 1) * 64], d_score))
        if head % 2 == 0:
            dv_pair, dk_pair = dv_sub, dk_sub
        else:
            dqkv[:, base:base + 128] = (jnp.concatenate(dq_parts, axis=0).T * 0.125).astype(BF)
            dqkv[:, d_model + base:d_model + base + 128] = (dk_pair + dk_sub).astype(BF)
            dqkv[:, 2 * d_model + base:2 * d_model + base + 128] = (dv_pair + dv_sub).astype(BF)
        now = following

    hid = h_ref[...].astype(F32)
    scale = rms_scale(hid)
    normed = (hid * scale).astype(BF)
    for part in range(3):
        cols = slice(part * d_model, (part + 1) * d_model)
        g_acc[:, cols] += dot(normed, dqkv[:, cols], TN)
    if with_input:
        ct_norm = dot(dqkv[...], w_ref[...], NT).astype(BF).astype(F32)
        ct_h_ref[...] = (ct_mid.astype(F32) + rms_pull(hid, scale, ct_norm)).astype(BF)

    @pl.when(last)
    def _():
        copy = pltpu.make_async_copy(g_acc, g_out, sems.at[len(loads)])
        copy.start()
        copy.wait()


def attn_backward(offsets, hidden, qkv, lse, ct_up, mid, ct, attn, bundle, w_qkv, with_input):
    seqs, seq_len = qkv.shape[:2]
    d_model, d_ff = hidden.shape[-1], ct_up.shape[-1]
    heads = d_model // 64
    blocks = bundle.shape[0]
    flops = 2 * seqs * seq_len * d_model * (d_ff + d_model * (8 if with_input else 5)) + 20 * seqs * heads * seq_len * seq_len * 128
    block = lambda width, which=None: pl.BlockSpec((None, seq_len, width), (lambda i, off: (i, 0, 0)) if which is None else (lambda i, off: (i + off[which] * seqs, 0, 0)))
    hbm = pl.BlockSpec(memory_space=pl.ANY)
    in_specs = [block(d_model, 0), block(3 * d_model), pl.BlockSpec((None, heads, seq_len), lambda i, off: (i, 0, 0)),
                block(d_ff), block(d_model), block(d_model, 1), block(d_model), hbm]
    args = [offsets, hidden, qkv, lse, ct_up, mid, ct, attn, bundle]
    out_specs = [hbm]
    out_shape = [jax.ShapeDtypeStruct((d_model, 4 * d_model), F32)]
    if with_input:
        in_specs.append(pl.BlockSpec((d_model, 3 * d_model), lambda i, off: (1, 0), pipeline_mode=pl.Buffered(1)))
        args.append(w_qkv)
        out_specs = [block(d_model)] + out_specs
        out_shape = [jax.ShapeDtypeStruct((seqs, seq_len, d_model), BF)] + out_shape
    return pl.pallas_call(
        functools.partial(attn_bwd_kernel, with_input),
        grid_spec=pltpu.PrefetchScalarGridSpec(
            num_scalar_prefetch=1,
            grid=(seqs,),
            in_specs=in_specs,
            out_specs=out_specs,
            scratch_shapes=[
                pltpu.VMEM((seq_len, d_model), BF),
                pltpu.VMEM((seq_len, 3 * d_model), BF),
                pltpu.VMEM((d_model, d_model), BF),
                pltpu.VMEM((d_model, d_ff), BF),
                pltpu.VMEM((d_model, 4 * d_model), F32),
                pltpu.SemaphoreType.DMA((blocks * (1 + d_ff // d_model) + 1,)),
            ],
        ),
        out_shape=out_shape,
        cost_estimate=pl.CostEstimate(flops=flops, bytes_accessed=50 << 20, transcendentals=0),
        compiler_params=pltpu.CompilerParams(vmem_limit_bytes=VMEM_LIMIT),
    )(*args)


def solution(mesh):
    stages = mesh.shape['pp']
    both = ('dp', 'pp')
    swap = [(0, 1), (1, 0)]

    def device_step(act_in, loss_seed, w_qkv, w_proj, w_up, w_down):
        stage = lax.axis_index('pp')
        micro = act_in.shape[0] // stages
        seq_len, d_model = act_in.shape[2:]
        d_ff = w_up.shape[2]
        ff_parts = d_ff // d_model
        seqs = micro * act_in.shape[1]
        tokens = seqs * seq_len
        own = stage.astype(jnp.int32).reshape(1)
        zero = jnp.zeros((1,), jnp.int32)

        wq_shard = w_qkv.reshape(-1, 3 * d_model)
        wq = lax.all_gather(wq_shard, ('pp', 'dp'), axis=0, tiled=True)
        w_proj, w_up, w_down, _ = lax.optimization_barrier((w_proj, w_up, w_down, wq_shard))

        rows = w_proj.shape[1] // 2
        mlp_halves = jnp.concatenate(
            [w_down[0].reshape(2, -1, d_model)]
            + [w_up[0, :, part * d_model:(part + 1) * d_model].reshape(2, rows, d_model) for part in range(ff_parts)]
            + [w_proj[0].reshape(2, rows, d_model)], axis=1)
        kept = lax.dynamic_index_in_dim(mlp_halves, stage, 0, keepdims=False)
        got = lax.ppermute(lax.dynamic_index_in_dim(mlp_halves, 1 - stage, 0, keepdims=False), 'pp', swap)
        bundles = []
        for layer in range(2):
            bundles.append(lax.all_gather(jnp.where(stage == layer, kept, got), both, axis=0))

        hidden = act_in.reshape(stages * seqs, seq_len, d_model)
        shape3 = (-1, seq_len, d_model)
        qkv, attn, lse = attn_forward(own, hidden, wq, 0, seqs)
        mid, up, out = mlp_forward(own, hidden.reshape(-1, d_model), attn.reshape(tokens, d_model), bundles[0], d_ff)
        first = (hidden, qkv, attn, lse, mid)

        hidden = out.reshape(shape3)
        qkv, attn, lse = attn_forward(zero, hidden, wq, 1, seqs)
        seed = loss_seed.reshape(stages * tokens, d_model)
        mid, ct_up, final_kept, final_sent, g_mlp = mlp_last(own, out, attn.reshape(tokens, d_model), seed, bundles[1], d_ff, seq_len)

        def reduce_rows(grad, layer):
            block = lax.psum_scatter(grad, both, scatter_dimension=0, tiled=True)
            got = lax.ppermute(block, 'pp', [(1 - layer, layer)])
            return (block, got) if layer == 0 else (got, block)

        def reduce_stage(grad, layer):
            block = lax.psum_scatter(grad, 'dp', scatter_dimension=0, tiled=True)
            got = lax.ppermute(block, 'pp', [(1 - layer, layer)])
            return block, got

        mlp_parts = [None, reduce_rows(g_mlp, 1)]
        attn_parts = [None, None]
        wide3 = (seqs, seq_len, d_ff)
        ct_h, g_attn = attn_backward(jnp.concatenate([zero, own]), hidden, qkv, lse, ct_up.reshape(wide3), mid.reshape(shape3), seed.reshape(shape3),
                                     attn, bundles[1], wq, True)
        attn_parts[1] = reduce_stage(g_attn, 1)

        hidden, qkv, attn, lse, mid = first
        ct_up, g_mlp = mlp_backward(zero, ct_h.reshape(tokens, d_model), up, mid, bundles[0])
        mlp_parts[0] = reduce_rows(g_mlp, 0)
        (g_attn,) = attn_backward(jnp.concatenate([own, zero]), hidden, qkv, lse, ct_up.reshape(wide3), mid.reshape(shape3), ct_h,
                                  attn, bundles[0], wq, False)
        attn_parts[0] = reduce_stage(g_attn, 0)

        half_shape = (micro, act_in.shape[1], seq_len // 2, d_model)
        got_down = lax.ppermute(final_sent, 'pp', [(1, 0)])
        got_up = lax.ppermute(final_sent, 'pp', [(0, 1)])
        final_kept, got_down, got_up = [out.reshape(half_shape) for out in (final_kept, got_down, got_up)]
        act_out = jnp.where(stage == 0, jnp.concatenate([final_kept, got_down]), jnp.concatenate([got_up, final_kept]))

        pick = lambda first, second: jnp.where(stage == 0, first, second)
        mlp = [pick(mlp_parts[0][half], mlp_parts[1][half]).reshape(-1, d_model) for half in range(2)]
        wide = pick(*[sum(parts) for parts in attn_parts])
        down = d_ff // (2 * mesh.shape['dp'])
        gd = jnp.concatenate([half[:down] for half in mlp])
        gu = jnp.concatenate([jnp.concatenate([half[down + part * rows:down + (part + 1) * rows] for part in range(ff_parts)], axis=1) for half in mlp])
        gq, gp = wide[:, :3 * d_model], wide[:, 3 * d_model:]
        return gq.reshape(w_qkv.shape), gp[None], gu[None], gd[None], act_out

    weight_spec = P('pp', 'dp')
    act_spec = P(None, 'dp')
    return jax.shard_map(device_step, mesh=mesh, in_specs=(act_spec, act_spec, weight_spec, weight_spec, weight_spec, weight_spec), out_specs=(weight_spec, weight_spec, weight_spec, weight_spec, P(None, 'dp', 'pp')), check_vma=False)
```
